32 devices in a mesh: seq: 2 (over core), heads: 4 (over y, x), batch: 4 (over z).
Axes of the slice: x: 2, y: 2, z: 4, core: 2. Of those that a mesh axis runs over, the one named last changes fastest.
Arguments:
- queries: bfloat16 [4, 512, 8192], P('batch', 'seq', 'heads'), may hold values from -160 to 160
- keys: bfloat16 [4, 512, 1024], P('batch', 'seq', 'heads'), may hold values from -7 to 7
- values: bfloat16 [4, 512, 1024], P('batch', 'seq', 'heads'), may hold values from -6 to 6
- doc_lengths: int32 [4, 16], P('batch'), may hold values from 1 to 384, 512 in all within a row
- out_weight: bfloat16 [8192, 8192], P('heads', 'batch'), may hold values from -0.0625 to 0.0625
Outputs:
- projected: bfloat16 [4, 512, 8192], P('heads', 'seq', 'batch')
The draws below stay inside these ranges and needn't reach their ends.
Inputs may be any that keep to these rules, and one draw needn't show every extreme that they name: `doc_lengths`: each row sums to 512; no document is longer than 384 tokens and one is exactly 384.
All inputs are finite; a program needn't handle non-finite values.
Results may differ from the reference program's by a relative error of at most 0.012.
Values may be sent and summed in bfloat16 or wider, within the bound.
A program may use at most 64 MiB of HBM per device.

```python
import math
import jax
import jax.numpy as jnp
import numpy as np
from jax import lax

QUERY_HEAD_COUNT = 64
VALUE_KEY_HEADS = 8
HEAD_WIDTH = 128
D = 8192
DOCS = 16
QBLOCK = 128
PACKED_BATCH = 4
PACKED_LENGTH = 512
LONGEST = 384


def shared_keys(key):
    sampled_values = jax.random.normal(jax.random.fold_in(key, 11), (PACKED_BATCH, PACKED_LENGTH, VALUE_KEY_HEADS, HEAD_WIDTH), jnp.float32)
    sampled_values = jnp.clip(sampled_values, -6.0, 6.0)
    return sampled_values


def draw_keys(key, part):
    sampled_values = shared_keys(key)
    return sampled_values.reshape(PACKED_BATCH, PACKED_LENGTH, VALUE_KEY_HEADS * HEAD_WIDTH).astype(jnp.bfloat16)


def draw_queries(key, part):
    sampled_values = jax.random.normal(jax.random.fold_in(key, 21), (PACKED_BATCH, PACKED_LENGTH, QUERY_HEAD_COUNT, HEAD_WIDTH), jnp.float32)
    sampled_values = jnp.clip(sampled_values, -6.0, 6.0)
    return sampled_values.reshape(PACKED_BATCH, PACKED_LENGTH, QUERY_HEAD_COUNT * HEAD_WIDTH).astype(jnp.bfloat16)


def level_of(stream_key, dims, shards, low, top_value):
    def one(dim, blocks):
        draws = jax.random.uniform(jax.random.fold_in(jax.random.fold_in(stream_key, 6), dim), (blocks,), jnp.float32, low / len(shards), top_value / len(shards))
        return jnp.repeat(jnp.exp(draws), dims[dim] // blocks).reshape((-1,) + (1,) * (len(dims) - dim - 1))

    loudness = one(*shards[0])
    for cut in shards[1:]:
        loudness = loudness * one(*cut)
    return loudness


def length_profile(count, total, limit, lean):
    portions = [(1 << 20) // math.isqrt(grade ** lean) + 1 for grade in range(2, count + 1)]
    rest, given = total - limit - (count - 1), [1] * (count - 1)
    while rest > 0:
        candidates = [i for i in range(count - 1) if given[i] < limit]
        whole, budget = sum([portions[i] for i in candidates]), rest
        for i in candidates:
            more = min(limit - given[i], max(1, budget * portions[i] // whole), rest)
            given[i] = given[i] + more
            rest = rest - more
    return np.array([limit] + given)


def ragged_sizes(key, count, total, bound, skew):
    if count == 2:
        one = jax.random.randint(key, (), max(1, total - bound), min(bound, total - 1) + 1)
        return jnp.stack([one, total - one])
    tallies = jnp.asarray(length_profile(count, total, bound, skew), jnp.int32)
    twos = (count - 1) // 2
    giver, receiver = tallies[1:1 + 2 * twos:2], tallies[2:2 + 2 * twos:2]
    margin = jnp.minimum(giver - 1, bound - receiver)
    shifted = jax.random.randint(jax.random.fold_in(key, 1), (twos,), 0, 1 << 20) % (margin + 1)
    tallies = tallies.at[1:1 + 2 * twos:2].set(giver - shifted).at[2:2 + 2 * twos:2].set(receiver + shifted)
    return tallies[jax.random.permutation(jax.random.fold_in(key, 2), count)]


def centred(own_key, dims, width, limit, pieces=(), held_as=jnp.bfloat16):
    entries = jax.random.normal(own_key, dims, jnp.float32) * width
    if len(pieces) > 0:
        entries = level_of(own_key, dims, pieces, -0.22, 0.18) * entries
    return jnp.clip(entries, min=-limit, max=limit).astype(held_as)


def setup_inputs(seed: int = 0) -> dict:
    arg_keys = jax.random.split(jax.random.key(seed), 6)
    queries = draw_queries(jax.random.fold_in(arg_keys[5], 71), 0)
    keys = draw_keys(jax.random.fold_in(arg_keys[5], 71), 0)
    values = centred(arg_keys[2], (PACKED_BATCH, PACKED_LENGTH, VALUE_KEY_HEADS * HEAD_WIDTH), 1.0, 6.0, ((0, 4), (1, 2), (2, 4)))
    doc_lengths = jax.vmap(lambda own: ragged_sizes(own, DOCS, PACKED_LENGTH, LONGEST, 2))(jax.random.split(arg_keys[3], PACKED_BATCH)).reshape((PACKED_BATCH, DOCS)).astype(jnp.int32)
    out_weight = centred(arg_keys[4], (QUERY_HEAD_COUNT * HEAD_WIDTH, D), (QUERY_HEAD_COUNT * HEAD_WIDTH) ** -0.5, 0.0625, ((0, 4), (1, 4)))
    return dict(queries=queries, keys=keys, values=values, doc_lengths=doc_lengths, out_weight=out_weight)


def document_of(lengths):
    doc_ends = jnp.cumsum(lengths)
    positions = jnp.arange(PACKED_LENGTH, dtype=jnp.int32)
    return jnp.sum((positions[:, None] >= doc_ends[None, :]).astype(jnp.int32), axis=1)


def attend_sequence(bundle):
    query_sequence, key_sequence, value_sequence, lengths = bundle
    group_width = QUERY_HEAD_COUNT // VALUE_KEY_HEADS
    key_span = min(LONGEST + QBLOCK, PACKED_LENGTH)
    doc_ids = document_of(lengths)
    query_head_rows = query_sequence.reshape(PACKED_LENGTH, VALUE_KEY_HEADS, group_width, HEAD_WIDTH)
    key_head_rows = key_sequence.reshape(PACKED_LENGTH, VALUE_KEY_HEADS, HEAD_WIDTH)
    value_head_rows = value_sequence.reshape(PACKED_LENGTH, VALUE_KEY_HEADS, HEAD_WIDTH)

    def one_block(block_index):
        q_start = (block_index * QBLOCK).astype(jnp.int32)
        k_start = jnp.clip(q_start + QBLOCK - key_span, 0, PACKED_LENGTH - key_span).astype(jnp.int32)
        q_block = lax.dynamic_slice_in_dim(query_head_rows, q_start, QBLOCK, 0).astype(jnp.float32)
        k_block = lax.dynamic_slice_in_dim(key_head_rows, k_start, key_span, 0).astype(jnp.float32)
        v_block = lax.dynamic_slice_in_dim(value_head_rows, k_start, key_span, 0).astype(jnp.float32)
        scores = jnp.einsum("qhgd,khd->hgqk", q_block, k_block, precision=lax.Precision.HIGHEST) * (HEAD_WIDTH ** -0.5)
        q_pos = q_start + jnp.arange(QBLOCK, dtype=jnp.int32)
        k_pos = k_start + jnp.arange(key_span, dtype=jnp.int32)
        q_doc = lax.dynamic_slice_in_dim(doc_ids, q_start, QBLOCK, 0)
        k_doc = lax.dynamic_slice_in_dim(doc_ids, k_start, key_span, 0)
        allowed = (q_doc[:, None] == k_doc[None, :]) & (k_pos[None, :] <= q_pos[:, None])
        scores = jnp.where(allowed, scores, -jnp.inf)
        highest = jnp.max(scores, axis=-1, keepdims=True)
        weights = jnp.exp(scores - highest)
        denominator = jnp.sum(weights, axis=-1)
        rounded = lax.optimization_barrier(weights.astype(jnp.bfloat16)).astype(jnp.float32)
        summed = jnp.einsum("hgqk,khd->qhgd", rounded, v_block, precision=lax.Precision.HIGHEST)
        result = summed / jnp.transpose(denominator, (2, 0, 1))[..., None]
        return result.reshape(QBLOCK, QUERY_HEAD_COUNT * HEAD_WIDTH).astype(jnp.bfloat16)

    outputs = lax.map(one_block, jnp.arange(PACKED_LENGTH // QBLOCK, dtype=jnp.int32))
    return outputs.reshape(PACKED_LENGTH, QUERY_HEAD_COUNT * HEAD_WIDTH)


def reference(queries, keys, values, doc_lengths, out_weight):
    attended = lax.map(attend_sequence, (queries, keys, values, doc_lengths))
    flat_rows = attended.reshape(PACKED_BATCH * PACKED_LENGTH, QUERY_HEAD_COUNT * HEAD_WIDTH).astype(jnp.float32)
    projected = jnp.dot(flat_rows, out_weight.astype(jnp.float32), precision=lax.Precision.HIGHEST)
    return projected.astype(jnp.bfloat16).reshape(PACKED_BATCH, PACKED_LENGTH, D)
```

```python
import functools

import jax
import jax.numpy as jnp
from jax import lax
from jax.experimental import pallas as pl
from jax.experimental.pallas import tpu as pltpu
from jax.sharding import PartitionSpec as P

HEAD_WIDTH = 128
DOCS = 16
PIECES = 4
LAG = 2
STACK = 4
COLS = 512
MESH = pl.DeviceIdType.MESH


def kernel(
    sizes, q_ref, k_ref, v_ref, len_ref, w_hbm, out_ref,
    w_ref, keys, vals, gath, stage, incoming,
    w_sem, kv_send, kv_recv, z_send, z_recv, c_send, c_recv,
):
    seqs, groups, n, reach = sizes
    shard_len, q_width = q_ref.shape[1], q_ref.shape[2]
    kv_heads = k_ref.shape[2] // HEAD_WIDTH
    per_kv = q_width // k_ref.shape[2]
    rows = shard_len // PIECES
    slots = n * PIECES
    half = w_ref.shape[1] // 2
    key_count = keys.shape[0]

    me = lax.axis_index("seq")
    head = lax.axis_index("heads")
    b = lax.axis_index("batch")

    def ring(h):
        return h + h // 2 - 2 * (h // 3) if groups == 4 else h

    place = ring(head)
    ahead = ring(lax.rem(place + 1, groups))
    behind = ring(lax.rem(place + groups - 1, groups))

    w_copy = pltpu.make_async_copy(w_hbm, w_ref, w_sem)
    w_copy.start()

    barrier = pltpu.get_barrier_semaphore()

    def greet(axis, index):
        pl.semaphore_signal(barrier, inc=1, device_id={axis: index}, device_id_type=MESH)

    greet("heads", ahead)
    greet("heads", behind)
    expected = 2
    for cond, index in ((b > 0, b - 1), (b < n - 1, b + 1)):
        expected = expected + cond.astype(jnp.int32)
        pl.when(cond)(functools.partial(greet, "batch", index))
    for d in range(1, reach + 1):
        for cond, index in ((me >= d, me - d), (me + d < seqs, me + d)):
            expected = expected + cond.astype(jnp.int32)
            pl.when(cond)(functools.partial(greet, "seq", index))
    pl.semaphore_wait(barrier, expected)

    def kv_copies(d, target):
        spot = pl.ds((reach - d) * shard_len, shard_len)
        return [
            pltpu.make_async_remote_copy(
                src_ref=src.at[0], dst_ref=dst.at[spot],
                send_sem=kv_send.at[i, d - 1], recv_sem=kv_recv.at[i, d - 1],
                device_id={"seq": target}, device_id_type=MESH,
            )
            for i, (src, dst) in enumerate(((k_ref, keys), (v_ref, vals)))
        ]

    for d in range(1, reach + 1):
        @pl.when(me + d < seqs)
        def _():
            for copy in kv_copies(d, me + d):
                copy.start()

    keys[pl.ds(reach * shard_len, shard_len), :] = k_ref[0]
    vals[pl.ds(reach * shard_len, shard_len), :] = v_ref[0]
    for d in range(1, reach + 1):
        @pl.when(me < d)
        def _():
            spot = pl.ds((reach - d) * shard_len, shard_len)
            keys[spot, :] = jnp.zeros((shard_len, keys.shape[1]), keys.dtype)
            vals[spot, :] = jnp.zeros((shard_len, vals.shape[1]), vals.dtype)

    for d in range(1, reach + 1):
        @pl.when(me >= d)
        def _():
            for copy in kv_copies(d, me - d):
                copy.wait_recv()

    def z_copy(way, source, piece):
        spot = pl.ds(pl.multiple_of(piece * rows, rows), rows)
        return pltpu.make_async_remote_copy(
            src_ref=gath.at[source, spot], dst_ref=gath.at[source, spot],
            send_sem=z_send.at[way, source, piece], recv_sem=z_recv.at[source, piece],
            device_id={"batch": b + 1 if way == 0 else b - 1}, device_id_type=MESH,
        )

    def goes(way, source):
        if way == 0:
            return (source <= b) & (b < n - 1)
        return (source >= b) & (b > 0)

    def pass_on(source, piece):
        for way in range(2):
            @pl.when(goes(way, source))
            def _():
                z_copy(way, source, piece).start()

    factor = HEAD_WIDTH ** (-0.5)
    shard_start = me * shard_len
    first_key = shard_start - reach * shard_len

    def attend(piece, _):
        base = pl.multiple_of(piece * rows, rows)
        row_pos = shard_start + base + lax.broadcasted_iota(jnp.int32, (rows, HEAD_WIDTH), 0)
        start = jnp.zeros((rows, HEAD_WIDTH), jnp.int32)
        end = jnp.int32(0)
        for d in range(DOCS):
            end = end + len_ref[0, d]
            start = jnp.where(row_pos >= end, end, start)
        key_pos = first_key + lax.broadcasted_iota(jnp.int32, (rows, key_count), 1)
        allowed = (key_pos >= start[:, :1]) & (key_pos <= row_pos[:, :1])
        bias = jnp.where(allowed, 0.0, -jnp.inf).astype(jnp.float32)
        bias = jnp.concatenate([bias] * STACK, axis=0)
        for first in range(0, kv_heads * per_kv, STACK):
            g = first // per_kv
            gcols = slice(g * HEAD_WIDTH, (g + 1) * HEAD_WIDTH)
            q = jnp.concatenate(
                [
                    q_ref[0, pl.ds(base, rows), j * HEAD_WIDTH:(j + 1) * HEAD_WIDTH]
                    for j in range(first, first + STACK)
                ],
                axis=0,
            )
            scores = lax.dot_general(
                q, keys[:, gcols], (((1,), (1,)), ((), ())),
                preferred_element_type=jnp.float32,
            ) * factor + bias
            weights = jnp.exp(scores - jnp.max(scores, axis=1, keepdims=True))
            total = jnp.sum(weights, axis=1, keepdims=True)
            summed = jnp.dot(
                weights.astype(jnp.bfloat16), vals[:, gcols],
                preferred_element_type=jnp.float32,
            )
            result = (summed / total).astype(jnp.bfloat16)
            for i in range(STACK):
                j = first + i
                gath[b, pl.ds(base, rows), j * HEAD_WIDTH:(j + 1) * HEAD_WIDTH] = (
                    result[i * rows:(i + 1) * rows]
                )
        pass_on(b, piece)
        return 0

    lax.fori_loop(0, PIECES, attend, 0)
    w_copy.wait()

    both = jnp.minimum(b, n - 1 - b)

    def slot_of(slot):
        u = jnp.maximum(slot - PIECES, 0)
        v = jnp.maximum(slot - PIECES - 2 * PIECES * both, 0)
        near_d = u // (2 * PIECES) + 1
        near_v = lax.rem(u, 2 * PIECES)
        near_seq = jnp.where(lax.rem(near_v, 2) == 0, b - near_d, b + near_d)
        far_d = both + 1 + v // PIECES
        far_seq = jnp.where(b > n - 1 - b, b - far_d, b + far_d)
        is_own = slot < PIECES
        is_near = slot < PIECES + 2 * PIECES * both
        seq = jnp.where(is_own, b, jnp.where(is_near, near_seq, far_seq))
        piece = jnp.where(is_own, slot, jnp.where(is_near, near_v // 2, lax.rem(v, PIECES)))
        return seq, piece

    def steps_from_root(way, source):
        gap = place - ring(source) if way == 0 else ring(source) - place
        return lax.rem(gap + groups, groups)

    def chain_copy(way, source, piece):
        return pltpu.make_async_remote_copy(
            src_ref=stage.at[way, source, piece], dst_ref=incoming.at[way, source, piece],
            send_sem=c_send.at[way, source, piece], recv_sem=c_recv.at[way, source, piece],
            device_id={"heads": ahead if way == 0 else behind}, device_id_type=MESH,
        )

    def hop(h, slot):
        source, piece = slot_of(slot)
        for way in range(2):
            @pl.when(steps_from_root(way, source) == (h + 1) % groups)
            def _():
                chain_copy(way, source, piece).wait_recv()
                merged = (
                    incoming[way, source, piece].astype(jnp.float32)
                    + stage[way, source, piece].astype(jnp.float32)
                ).astype(jnp.bfloat16)
                if h < groups - 1:
                    stage[way, source, piece] = merged
                    chain_copy(way, source, piece).start()
                else:
                    spot = pl.ds(pl.multiple_of(piece * rows, rows), rows)
                    out_ref[0, spot, way * half:(way + 1) * half] = merged

    def step(i, _):
        @pl.when(i < slots)
        def _():
            source, piece = slot_of(i)

            @pl.when(source != b)
            def _():
                z_copy(0, source, piece).wait_recv()
                pass_on(source, piece)

            spot = pl.ds(pl.multiple_of(piece * rows, rows), rows)
            for way in range(2):
                def tile(t, _):
                    cols = pl.multiple_of(t * COLS, COLS)
                    stage[way, source, piece, :, pl.ds(cols, COLS)] = jnp.dot(
                        gath[source, spot, :],
                        w_ref[:, pl.ds(pl.multiple_of(way * half + cols, COLS), COLS)],
                        preferred_element_type=jnp.float32,
                    ).astype(jnp.bfloat16)
                    return 0

                lax.fori_loop(0, half // COLS, tile, 0)

                @pl.when(steps_from_root(way, source) == 1)
                def _():
                    chain_copy(way, source, piece).start()

        for h in range(1, groups):
            slot = i - h * LAG

            @pl.when((slot >= 0) & (slot < slots))
            def _():
                hop(h, slot)

        return 0

    lax.fori_loop(0, slots + (groups - 1) * LAG, step, 0)

    for d in range(1, reach + 1):
        @pl.when(me + d < seqs)
        def _():
            for copy in kv_copies(d, me + d):
                copy.wait_send()

    def finish(slot, _):
        source, piece = slot // PIECES, lax.rem(slot, PIECES)
        for way in range(2):
            @pl.when(goes(way, source))
            def _():
                z_copy(way, source, piece).wait_send()

            @pl.when(steps_from_root(way, source) != 0)
            def _():
                chain_copy(way, source, piece).wait_send()

        return 0

    lax.fori_loop(0, slots, finish, 0)


def solution(mesh):
    seqs, groups, n = mesh.shape["seq"], mesh.shape["heads"], mesh.shape["batch"]

    def per_device(queries, keys, values, doc_lengths, out_weight):
        shard_len, q_width = queries.shape[1:]
        kv_width = keys.shape[2]
        columns = out_weight.shape[1]
        seq_total = seqs * shard_len
        longest = seq_total // 2 + shard_len // 2
        reach = min((longest + shard_len - 2) // shard_len, seqs - 1)
        rows = shard_len // PIECES
        key_count = (reach + 1) * shard_len
        vmem = pl.BlockSpec(memory_space=pltpu.VMEM)
        dma = pltpu.SemaphoreType.DMA
        return pl.pallas_call(
            functools.partial(kernel, (seqs, groups, n, reach)),
            out_shape=jax.ShapeDtypeStruct((1, shard_len, columns), jnp.bfloat16),
            in_specs=[
                vmem, vmem, vmem,
                pl.BlockSpec(memory_space=pltpu.SMEM),
                pl.BlockSpec(memory_space=pl.ANY),
            ],
            out_specs=vmem,
            scratch_shapes=[
                pltpu.VMEM(out_weight.shape, jnp.bfloat16),
                pltpu.VMEM((key_count, kv_width), jnp.bfloat16),
                pltpu.VMEM((key_count, kv_width), jnp.bfloat16),
                pltpu.VMEM((n, shard_len, q_width), jnp.bfloat16),
                pltpu.VMEM((2, n, PIECES, rows, columns // 2), jnp.bfloat16),
                pltpu.VMEM((2, n, PIECES, rows, columns // 2), jnp.bfloat16),
                dma,
                dma((2, max(reach, 1))),
                dma((2, max(reach, 1))),
                dma((2, n, PIECES)),
                dma((n, PIECES)),
                dma((2, n, PIECES)),
                dma((2, n, PIECES)),
            ],
            compiler_params=pltpu.CompilerParams(
                collective_id=0, has_side_effects=True, vmem_limit_bytes=60 * 2**20
            ),
        )(queries, keys, values, doc_lengths, out_weight)

    return jax.shard_map(
        per_device,
        mesh=mesh,
        in_specs=(
            P("batch", "seq", "heads"),
            P("batch", "seq", "heads"),
            P("batch", "seq", "heads"),
            P("batch", None),
            P("heads", "batch"),
        ),
        out_specs=P("heads", "seq", "batch"),
        check_vma=False,
    )
```
